32 devices in a mesh: snap: 2 (over core), shard: 16 (over z, y, x).
Axes of the slice: x: 2, y: 2, z: 4, core: 2. Of those that a mesh axis runs over, the one named last changes fastest.
Arguments:
- snapshots: float32 [32, 524288], P(('snap', 'shard')), may hold values from -6 to 6
- coefficients: float32 [32], P(('snap', 'shard')), may hold values from -1 to 1
Outputs:
- synthesized: float32 [524288], P('shard')
The draws below stay inside these ranges and needn't reach their ends.
All inputs are finite; a program needn't handle non-finite values.
Results may differ from the reference program's by a relative error of at most 0.000078.
Values sent between devices are 32-bit elements; how exact they have to be, the bound alone decides.
A program may use at most 64 MiB of HBM per device.

```python
import jax
import jax.numpy as jnp
from jax import lax

PARAMS = 524288
SNAPSHOTS = 32


def raised(values, own_key, source, target, shards_of, factor):
    def block_of(dim):
        return (jnp.arange(values.shape[dim]) // (values.shape[dim] // shards_of)).reshape((-1,) + (1,) * (values.ndim - 1 - dim))

    one_side = jax.random.permutation(own_key, shards_of)[block_of(target)]
    second = (block_of(target) + shards_of // 2) % shards_of
    return jnp.where((block_of(source) == one_side) | (block_of(source) == second), factor * values, values)


def level_of(rng, shape, pieces, low, largest):
    level = 1.0
    for dim, blocks in pieces:
        heights = jax.random.uniform(jax.random.fold_in(jax.random.fold_in(rng, 6), dim), (blocks,), jnp.float32, low / len(pieces), largest / len(pieces))
        level = level * jnp.repeat(jnp.exp(heights), shape[dim] // blocks).reshape((-1,) + (1,) * (len(shape) - 1 - dim))
    return level


def scatter_about(key, shape, spread, limit, split=(), held_as=jnp.bfloat16):
    drawn = spread * jax.random.normal(key, shape, jnp.float32)
    if split:
        drawn = drawn * level_of(key, shape, split, -0.22, 0.18)
    return jnp.clip(drawn, -limit, limit).astype(held_as)


def gaussian_with(own_key, extent, deviation, bound, pieces, heavy, kind=jnp.bfloat16):
    result = deviation * jax.random.normal(own_key, extent, jnp.float32)
    if pieces:
        result = result * level_of(own_key, extent, pieces, -0.22, 0.18)
    return jnp.clip(raised(result, jax.random.fold_in(own_key, 3), *heavy), -bound, bound).astype(kind)


def setup_inputs(seed: int = 0) -> dict:
    key_list = jax.random.split(jax.random.key(seed), 3)
    return {
        "snapshots": gaussian_with(key_list[0], (SNAPSHOTS, PARAMS), 1.0, 6.0, ((0, 32),), (0, 1, 32, 2.75), jnp.float32),
        "coefficients": scatter_about(key_list[1], (SNAPSHOTS,), 0.0625, 1.0, ((0, 32),), jnp.float32),
    }


def reference(snapshots, coefficients):
    return jnp.dot(coefficients, snapshots, precision=lax.Precision.HIGHEST, preferred_element_type=jnp.float32)
```

```python
import functools

import jax
import jax.numpy as jnp
from jax import lax
from jax.experimental import pallas as pl
from jax.experimental.pallas import tpu as pltpu
from jax.sharding import PartitionSpec as P

MESH = pl.DeviceIdType.MESH
LANES = 128
TILE = 8
CHUNK = 128
PLAN = ((0, 4, 0), (1, 7, 0), (2, 5, 0))


def strides_of(size):
    return tuple(1 << b for b in range(size.bit_length() - 1))


def parts_of(rows, shard_strides):
    tiles = rows // TILE
    whole = sum(share for _, share, _ in PLAN)
    parts, done, seen = [], 0, 0
    for turn, share, wave in PLAN:
        seen += share
        upto = tiles * seen // whole
        if upto > done:
            head = list(shard_strides[:3])
            turn = turn % max(len(head), 1)
            order = head[turn:] + head[:turn] + list(shard_strides[3:])
            parts.append((tuple(order), done * TILE, (upto - done) * TILE, wave))
        done = upto
    return tuple(parts)


def kernel(parts, n, m, coef, snap, out, stage, work, got,
           load_sem, send_sem, recv_sem, share_send, share_recv):
    snap_id = lax.axis_index("snap")
    shard_id = lax.axis_index("shard")
    snap_strides, shard_strides = strides_of(m), strides_of(n)

    def step_of(index, stride):
        return stride - 2 * stride * lax.rem(lax.div(index, stride), 2)

    steps = {("snap", s): step_of(snap_id, s) for s in snap_strides}
    steps.update({("shard", s): step_of(shard_id, s) for s in shard_strides})

    def moved(axis, strides):
        index = snap_id if axis == "snap" else shard_id
        for s in strides:
            index = index + steps[axis, s]
        return index

    def partner(axis, stride):
        if axis == "snap":
            return (moved("snap", (stride,)), shard_id)
        return (snap_id, moved("shard", (stride,)))

    def bits_set(number):
        return tuple(s for s in snap_strides if number & s)

    levels = [
        [("snap", s) for s in snap_strides] + [("shard", s) for s in order]
        for order, _, _, _ in parts
    ]
    depth = len(levels[0])
    blocks = n * m

    loads = []
    for p, (_, first, rows, _) in enumerate(parts):
        load = pltpu.make_async_copy(
            snap.at[:, :, pl.ds(first, rows), :], stage.at[:, :, pl.ds(first, rows), :], load_sem.at[p]
        )
        load.start()
        loads.append(load)

    barrier = pltpu.get_barrier_semaphore()
    peers = [(moved("snap", bits_set(d)), shard_id) for d in range(1, m)]
    peers += [partner("shard", s) for s in shard_strides]
    for peer in peers:
        pl.semaphore_signal(barrier, inc=1, device_id=peer, device_id_type=MESH)

    scale = coef[0]
    sends = []

    def copy_of(p, level):
        _, first, rows, _ = parts[p]
        half = (blocks >> (level + 1)) * rows
        span = pl.ds(blocks * first + half, half)
        return pltpu.make_async_remote_copy(
            src_ref=work.at[span, :],
            dst_ref=got.at[span, :],
            send_sem=send_sem.at[p * depth + level],
            recv_sem=recv_sem.at[p * depth + level],
            device_id=partner(*levels[p][level]),
            device_id_type=MESH,
        )

    copies = {(p, level): copy_of(p, level) for p in range(len(parts)) for level in range(depth)}

    def weigh(p, positions):
        _, first, rows, _ = parts[p]
        for position in positions:
            taken = [levels[p][k] for k in range(depth) if (position >> (depth - 1 - k)) & 1]
            owner = moved("shard", [s for axis, s in taken if axis == "shard"])
            part = moved("snap", [s for axis, s in taken if axis == "snap"])
            work[pl.ds(blocks * first + position * rows, rows), :] = (
                scale * stage[owner, part, pl.ds(first, rows), :]
            )

    def accumulate(p, level, upper):
        _, first, rows, _ = parts[p]
        half = (blocks >> (level + 1)) * rows
        quarter = half // 2
        base, source = blocks * first + (quarter if upper else 0), half
        for at in range(0, quarter, CHUNK):
            count = min(CHUNK, quarter - at)
            here = pl.ds(base + at, count)
            there = pl.ds(base + source + at, count)
            work[here, :] = work[here, :] + got[there, :]

    for p in range(len(parts)):
        loads[p].wait()
        weigh(p, range(blocks // 2, blocks))
        if p == 0:
            pl.semaphore_wait(barrier, len(peers))
        copies[p, 0].start()
        weigh(p, range(blocks // 2))

    shares = []
    todo = [(level + parts[p][3], level, p) for level in range(1, depth + 1) for p in range(len(parts))]
    for _, level, p in sorted(todo):
        _, first, rows, _ = parts[p]
        copies[p, level - 1].wait_recv()
        if level < depth:
            accumulate(p, level - 1, True)
            copies[p, level].start()
            accumulate(p, level - 1, False)
        else:
            base = blocks * first
            out[snap_id, pl.ds(first, rows), :] = work[pl.ds(base, rows), :] + got[pl.ds(base + rows, rows), :]
            for d in range(1, m):
                share = pltpu.make_async_remote_copy(
                    src_ref=out.at[snap_id, pl.ds(first, rows), :],
                    dst_ref=out.at[snap_id, pl.ds(first, rows), :],
                    send_sem=share_send.at[p * m + d],
                    recv_sem=share_recv.at[p * m + d],
                    device_id=(moved("snap", bits_set(d)), shard_id),
                    device_id_type=MESH,
                )
                share.start()
                shares.append(share)

    for share in shares:
        share.wait_recv()
    for copy in copies.values():
        copy.wait_send()
    for share in shares:
        share.wait_send()


def by_collectives(snapshots, coefficients):
    total = jnp.sum(coefficients[:, None] * snapshots, axis=0)
    return lax.psum(lax.psum_scatter(total, "shard", scatter_dimension=0, tiled=True), "snap")


def per_device(n, m, snapshots, coefficients):
    count, params = snapshots.shape
    power = n & (n - 1) == 0 and m & (m - 1) == 0 and n * m > 1
    if count != 1 or not power or params % (n * m * TILE * LANES):
        return by_collectives(snapshots, coefficients)
    rows = params // (n * m * LANES)
    parts = parts_of(rows, strides_of(n))
    depth = len(strides_of(n)) + len(strides_of(m))
    result = pl.pallas_call(
        functools.partial(kernel, parts, n, m),
        out_shape=jax.ShapeDtypeStruct((m, rows, LANES), jnp.float32),
        in_specs=[pl.BlockSpec(memory_space=pltpu.SMEM), pl.BlockSpec(memory_space=pl.ANY)],
        out_specs=pl.BlockSpec(memory_space=pltpu.VMEM),
        scratch_shapes=[
            pltpu.VMEM((n, m, rows, LANES), jnp.float32),
            pltpu.VMEM((n * m * rows, LANES), jnp.float32),
            pltpu.VMEM((n * m * rows, LANES), jnp.float32),
            pltpu.SemaphoreType.DMA((len(parts),)),
            pltpu.SemaphoreType.DMA((len(parts) * depth,)),
            pltpu.SemaphoreType.DMA((len(parts) * depth,)),
            pltpu.SemaphoreType.DMA((len(parts) * m,)),
            pltpu.SemaphoreType.DMA((len(parts) * m,)),
        ],
        compiler_params=pltpu.CompilerParams(collective_id=0, has_side_effects=True),
    )(coefficients, snapshots.reshape(n, m, rows, LANES))
    return result.reshape(params // n)


def solution(mesh):
    n, m = mesh.shape["shard"], mesh.shape["snap"]
    return jax.shard_map(
        functools.partial(per_device, n, m),
        mesh=mesh,
        in_specs=(P(("snap", "shard"), None), P(("snap", "shard"))),
        out_specs=P("shard"),
        check_vma=False,
    )
```

```python
import functools

import jax
import jax.numpy as jnp
from jax import lax
from jax.experimental import pallas as pl
from jax.experimental.pallas import tpu as pltpu
from jax.sharding import PartitionSpec as P

MESH = pl.DeviceIdType.MESH
LANES = 128
TILE = 8
CHUNK = 128
PLAN = (
    ((1, 0, 3, 2), 3, (0, 7, 14, 24, 29)),
    ((0, 3, 1, 2), 3, (1, 8, 19, 25, 31)),
    ((2, 1, 0, 3), 3, (2, 9, 15, 21, 28)),
    ((0, 2, 1, 3), 2, (3, 11, 17, 23, 32)),
    ((2, 0, 3, 1), 2, (4, 12, 18, 27, 34)),
    ((1, 0, 2, 3), 2, (5, 10, 16, 22, 30)),
    ((1, 3, 0, 2), 1, (6, 13, 20, 26, 33)),
)


def strides_of(size):
    return tuple(1 << b for b in range(size.bit_length() - 1))


def parts_of(rows, shard_strides):
    tiles = rows // TILE
    whole = sum(share for _, share, _ in PLAN)
    parts, done, seen = [], 0, 0
    for turn, share, ranks in PLAN:
        seen += share
        upto = tiles * seen // whole
        if upto > done:
            order = [shard_strides[b] for b in turn if b < len(shard_strides)]
            order += shard_strides[len(order):]
            parts.append((tuple(order), done * TILE, (upto - done) * TILE, ranks))
        done = upto
    return tuple(parts)


def kernel(parts, n, m, coef, snap, out, stage, work, got,
           load_sem, send_sem, recv_sem, share_send, share_recv):
    snap_id = lax.axis_index("snap")
    shard_id = lax.axis_index("shard")
    snap_strides, shard_strides = strides_of(m), strides_of(n)

    def step_of(index, stride):
        return stride - 2 * stride * lax.rem(lax.div(index, stride), 2)

    steps = {("snap", s): step_of(snap_id, s) for s in snap_strides}
    steps.update({("shard", s): step_of(shard_id, s) for s in shard_strides})

    def moved(axis, strides):
        index = snap_id if axis == "snap" else shard_id
        for s in strides:
            index = index + steps[axis, s]
        return index

    def partner(axis, stride):
        if axis == "snap":
            return (moved("snap", (stride,)), shard_id)
        return (snap_id, moved("shard", (stride,)))

    def bits_set(number):
        return tuple(s for s in snap_strides if number & s)

    levels = [
        [("snap", s) for s in snap_strides] + [("shard", s) for s in order]
        for order, _, _, _ in parts
    ]
    depth = len(levels[0])
    blocks = n * m

    loads = []
    for p, (_, first, rows, _) in enumerate(parts):
        span = pl.ds(first, rows)
        load = pltpu.make_async_copy(snap.at[:, :, span, :], stage.at[:, :, span, :], load_sem.at[p])
        load.start()
        loads.append(load)

    barrier = pltpu.get_barrier_semaphore()
    peers = [(moved("snap", bits_set(d)), shard_id) for d in range(1, m)]
    peers += [partner("shard", s) for s in shard_strides]
    for peer in peers:
        pl.semaphore_signal(barrier, inc=1, device_id=peer, device_id_type=MESH)

    scale = coef[0]
    sends = []

    def copy_of(p, level):
        _, first, rows, _ = parts[p]
        half = (blocks >> (level + 1)) * rows
        span = pl.ds(blocks * first + half, half)
        return pltpu.make_async_remote_copy(
            src_ref=work.at[span, :],
            dst_ref=got.at[span, :],
            send_sem=send_sem.at[p * depth + level],
            recv_sem=recv_sem.at[p * depth + level],
            device_id=partner(*levels[p][level]),
            device_id_type=MESH,
        )

    copies = {(p, level): copy_of(p, level) for p in range(len(parts)) for level in range(depth)}

    def weigh(p, positions):
        _, first, rows, _ = parts[p]
        for position in positions:
            taken = [levels[p][k] for k in range(depth) if (position >> (depth - 1 - k)) & 1]
            owner = moved("shard", [s for axis, s in taken if axis == "shard"])
            part = moved("snap", [s for axis, s in taken if axis == "snap"])
            work[pl.ds(blocks * first + position * rows, rows), :] = (
                scale * stage[owner, part, pl.ds(first, rows), :]
            )

    def accumulate(p, level, upper):
        _, first, rows, _ = parts[p]
        half = (blocks >> (level + 1)) * rows
        quarter = half // 2
        base, source = blocks * first + (quarter if upper else 0), half
        for at in range(0, quarter, CHUNK):
            count = min(CHUNK, quarter - at)
            here = pl.ds(base + at, count)
            there = pl.ds(base + source + at, count)
            work[here, :] = work[here, :] + got[there, :]

    for p in range(len(parts)):
        loads[p].wait()
        weigh(p, range(blocks // 2, blocks))
        if p == 0:
            pl.semaphore_wait(barrier, len(peers))
        copies[p, 0].start()
        weigh(p, range(blocks // 2))

    shares = []
    extra = depth - len(PLAN[0][2])
    todo = [
        (ranks[max(level - 1 - extra, 0)], level, p)
        for p, (_, _, _, ranks) in enumerate(parts)
        for level in range(1, depth + 1)
    ]
    for _, level, p in sorted(todo):
        _, first, rows, _ = parts[p]
        copies[p, level - 1].wait_recv()
        if level < depth:
            accumulate(p, level - 1, True)
            copies[p, level].start()
            accumulate(p, level - 1, False)
        else:
            base = blocks * first
            out[snap_id, pl.ds(first, rows), :] = work[pl.ds(base, rows), :] + got[pl.ds(base + rows, rows), :]
            for d in range(1, m):
                share = pltpu.make_async_remote_copy(
                    src_ref=out.at[snap_id, pl.ds(first, rows), :],
                    dst_ref=out.at[snap_id, pl.ds(first, rows), :],
                    send_sem=share_send.at[p * m + d],
                    recv_sem=share_recv.at[p * m + d],
                    device_id=(moved("snap", bits_set(d)), shard_id),
                    device_id_type=MESH,
                )
                share.start()
                shares.append(share)

    for share in shares:
        share.wait_recv()
    for copy in copies.values():
        copy.wait_send()
    for share in shares:
        share.wait_send()


def by_collectives(snapshots, coefficients):
    total = jnp.sum(coefficients[:, None] * snapshots, axis=0)
    return lax.psum(lax.psum_scatter(total, "shard", scatter_dimension=0, tiled=True), "snap")


def per_device(n, m, snapshots, coefficients):
    count, params = snapshots.shape
    power = n & (n - 1) == 0 and m & (m - 1) == 0 and n * m > 1
    if count != 1 or not power or params % (n * m * TILE * LANES):
        return by_collectives(snapshots, coefficients)
    rows = params // (n * m * LANES)
    parts = parts_of(rows, strides_of(n))
    depth = len(strides_of(n)) + len(strides_of(m))
    result = pl.pallas_call(
        functools.partial(kernel, parts, n, m),
        out_shape=jax.ShapeDtypeStruct((m, rows, LANES), jnp.float32),
        in_specs=[pl.BlockSpec(memory_space=pltpu.SMEM), pl.BlockSpec(memory_space=pltpu.HBM)],
        out_specs=pl.BlockSpec(memory_space=pltpu.VMEM),
        scratch_shapes=[
            pltpu.VMEM((n, m, rows, LANES), jnp.float32),
            pltpu.VMEM((n * m * rows, LANES), jnp.float32),
            pltpu.VMEM((n * m * rows, LANES), jnp.float32),
            pltpu.SemaphoreType.DMA((len(parts),)),
            pltpu.SemaphoreType.DMA((len(parts) * depth,)),
            pltpu.SemaphoreType.DMA((len(parts) * depth,)),
            pltpu.SemaphoreType.DMA((len(parts) * m,)),
            pltpu.SemaphoreType.DMA((len(parts) * m,)),
        ],
        compiler_params=pltpu.CompilerParams(collective_id=0, has_side_effects=True, vmem_limit_bytes=52 * 1024 * 1024),
    )(coefficients, snapshots.reshape(n, m, rows, LANES))
    return result.reshape(params // n)


def solution(mesh):
    n, m = mesh.shape["shard"], mesh.shape["snap"]
    return jax.shard_map(
        functools.partial(per_device, n, m),
        mesh=mesh,
        in_specs=(P(("snap", "shard"), None), P(("snap", "shard"))),
        out_specs=P("shard"),
        check_vma=False,
    )
```
